32 devices in a mesh: shot: 8 (over z, y), depth: 4 (over x, core).
Axes of the slice: x: 2, y: 2, z: 4, core: 2. Of those that a mesh axis runs over, the one named last changes fastest.
Arguments:
- correlation: float32 [16, 16, 32, 512], P('shot', None, None, 'depth'), may hold values from -6 to 6
- illumination: float32 [16, 16, 32, 512], P('shot', None, None, 'depth'), may hold values from 0.25 to 4
- aperture: int32 [16, 4], P('shot'), may hold values from 0 to 32, as said below
Outputs:
- stack: float32 [16, 32, 512], P('shot', None, 'depth')
The draws below stay inside these ranges and needn't reach their ends.
Inputs may be any that keep to these rules, and one draw needn't show every extreme that they name: For every shot, 0 <= aperture[s,0] < aperture[s,1] <= 16 and 0 <= aperture[s,2] < aperture[s,3] <= 32; each box spans a quarter to a half of the grid along each of the two dimensions.
All inputs are finite; a program needn't handle non-finite values.
Results may differ from the reference program's by a relative error of at most 0.0003.
Values sent between devices are 32-bit elements.
A program may use at most 64 MiB of HBM per device.

```python
import math
import jax
import jax.numpy as jnp
from jax import lax

NY = 32
SHOTS = 16
NX = 16
NZ = 512


def draw_aperture(key, part):
    key_first = jax.random.fold_in(key, 11)
    key_second = jax.random.fold_in(key, 23)
    k_one, k_two = jax.random.split(key_first)
    k_three, k_four = jax.random.split(key_second)
    low_first = jax.random.randint(k_one, (SHOTS,), 0, NX // 2)
    span_first = jax.random.randint(k_two, (SHOTS,), max(NX // 4, 1), NX // 2 + 1)
    low_second = jax.random.randint(k_three, (SHOTS,), 0, NY // 2)
    span_second = jax.random.randint(k_four, (SHOTS,), max(NY // 4, 1), NY // 2 + 1)
    return jnp.stack([low_first, low_first + span_first, low_second, low_second + span_second], axis=1).astype(jnp.int32)


def spiked(values, rng, source, target, blocks, factor):
    owner, partner = [(jnp.arange(values.shape[position]) // (values.shape[position] // blocks)).reshape([-1 if axis == position else 1 for axis in range(values.ndim)]) for position in (source, target)]
    chosen = jax.random.permutation(rng, blocks)[partner]
    strong = (owner == chosen) | (owner == (partner + blocks // 2) % blocks)
    return jnp.where(strong, factor * values, values)


def steps_of(stream_key, dims, pieces, smallest, high):
    def one(dim, blocks):
        draws = jax.random.uniform(jax.random.fold_in(jax.random.fold_in(stream_key, 6), dim), (blocks,), jnp.float32, smallest / len(pieces), high / len(pieces))
        return jnp.repeat(jnp.exp(draws), dims[dim] // blocks).reshape((-1,) + (1,) * (len(dims) - dim - 1))

    gain = one(*pieces[0])
    for cut in pieces[1:]:
        gain = gain * one(*cut)
    return gain


def gaussian_with(stream_key, dims, width, most, pieces, heavy, kind=jnp.bfloat16):
    array = width * jax.random.normal(stream_key, dims, jnp.float32)
    if pieces:
        array = array * steps_of(stream_key, dims, pieces, -0.22, 0.18)
    return jnp.clip(spiked(array, jax.random.fold_in(stream_key, 3), *heavy), -most, most).astype(kind)


def setup_inputs(seed: int = 0) -> dict:
    seeds = jax.random.split(jax.random.key(seed), 4)
    correlation = gaussian_with(seeds[0], (SHOTS, NX, NY, NZ), 1.0, 6.0, ((0, 8), (3, 4)), (0, 1, 8, 2.0), jnp.float32)
    illumination = jnp.clip(jnp.exp(math.log(4.0) - 2.7725887 * jax.random.uniform(seeds[1], (SHOTS, NX, NY, NZ), jnp.float32) ** steps_of(seeds[1], (SHOTS, NX, NY, NZ), ((0, 8), (3, 4)), -0.2, 0.2)), 0.25, 4.0)
    aperture = draw_aperture(jax.random.fold_in(seeds[3], 71), 0)
    return {"correlation": correlation, "illumination": illumination, "aperture": aperture}


def negative_laplacian(field):
    padded = jnp.pad(field, 1)
    beside = padded[2:, 1:-1, 1:-1] + padded[:-2, 1:-1, 1:-1]
    beside = beside + padded[1:-1, 2:, 1:-1] + padded[1:-1, :-2, 1:-1]
    beside = beside + padded[1:-1, 1:-1, 2:] + padded[1:-1, 1:-1, :-2]
    return 6.0 * field - beside

def prepare(correlation, illumination, box):
    first = lax.broadcasted_iota(jnp.int32, (NX, NY, 1), 0)
    second = lax.broadcasted_iota(jnp.int32, (NX, NY, 1), 1)
    inside = (first >= box[0]) & (first < box[1]) & (second >= box[2]) & (second < box[3])
    mask = inside.astype(jnp.float32)
    return negative_laplacian(mask * correlation / (illumination + 0.1))

def reference(correlation, illumination, aperture):
    cells = NX * NY * NZ

    def energy(items):
        filtered = prepare(items[0], items[1], items[2])
        return jnp.sum(filtered * filtered) / cells
    meansq = lax.map(energy, (correlation, illumination, aperture))
    peak = jnp.max(meansq)
    weight = 1.0 / jnp.sqrt(meansq + 0.5 * peak + 1.0)

    def accumulate(total, items):
        filtered = prepare(items[0], items[1], items[2])
        return (total + items[3] * filtered, None)
    stack, unused = lax.scan(accumulate, jnp.zeros((NX, NY, NZ), jnp.float32), (correlation, illumination, aperture, weight))
    return stack / jnp.sqrt(jnp.float32(SHOTS))
```

```python
import functools
import math

import jax
import jax.numpy as jnp
from jax import lax
from jax.experimental import pallas as pl
from jax.experimental.pallas import tpu as pltpu
from jax.sharding import PartitionSpec as P

MESH = pl.DeviceIdType.MESH
LANES = 128
SUBLANES = 8


def kernel(dims, corr_hbm, ill_hbm, box, out_ref, corr, ill, norm, halo_out, halo_in, send, recv,
           energy_out, energy_in, note_out, note_in, load_sem, halo_sem, bulk_send, bulk_recv,
           energy_send, energy_recv, note_send, note_recv):
    shots, rows, cols, slab, groups, slabs, owned, width, total_shots, cells = dims
    tiles = cols // SUBLANES
    per_row = shots * tiles
    rows_per_pack = LANES // per_row
    packs = rows // rows_per_pack
    group = lax.axis_index("shot")
    depth = lax.axis_index("depth")

    loads = []
    for s in range(shots):
        pair = (
            pltpu.make_async_copy(corr_hbm.at[s], corr.at[s], load_sem.at[0, s]),
            pltpu.make_async_copy(ill_hbm.at[s], ill.at[s], load_sem.at[1, s]),
        )
        for copy in pair:
            copy.start()
        loads.append(pair)

    barrier = pltpu.get_barrier_semaphore()
    for j in range(1, slabs):
        pl.semaphore_signal(barrier, inc=1, device_id={"depth": lax.rem(depth + j, slabs)}, device_id_type=MESH)
    for j in range(1, groups):
        pl.semaphore_signal(barrier, inc=1, device_id={"shot": lax.rem(group + j, groups)}, device_id_type=MESH)

    lane = lax.broadcasted_iota(jnp.int32, (SUBLANES, LANES), 1)
    lane_row = lax.broadcasted_iota(jnp.int32, (cols, slab), 1)
    col = lax.broadcasted_iota(jnp.int32, (cols, slab), 0)
    plane = jnp.zeros((cols, slab), jnp.float32)
    edge = jnp.zeros((SUBLANES, slab), jnp.float32)
    for s in range(shots):
        norm[s, 0, pl.ds(SUBLANES, cols)] = plane
        norm[s, rows + 1, pl.ds(SUBLANES, cols)] = plane

    col_mask = [(col >= box[s, 2]) & (col < box[s, 3]) for s in range(shots)]
    for pair in loads:
        for copy in pair:
            copy.wait()

    def normalise(p, carry):
        low = edge
        high = edge
        for i in range(rows_per_pack):
            r = p * rows_per_pack + i
            for s in range(shots):
                inside = col_mask[s] & (r >= box[s, 0]) & (r < box[s, 1])
                value = jnp.where(inside, corr[s, r], 0.0) / (ill[s, r] + 0.1)
                norm[s, r + 1, pl.ds(0, SUBLANES)] = edge
                norm[s, r + 1, pl.ds(SUBLANES, cols)] = value
                norm[s, r + 1, pl.ds(SUBLANES + cols, SUBLANES)] = edge
                for c in range(tiles):
                    k = (i * shots + s) * tiles + c
                    piece = value[c * SUBLANES:(c + 1) * SUBLANES]
                    low = jnp.where(lane == k, pltpu.roll(piece, k, 1), low)
                    high = jnp.where(lane == k, pltpu.roll(piece, (k + 1) % LANES, 1), high)
        halo_out[0, p] = low
        halo_out[1, p] = high
        return carry

    lax.fori_loop(0, packs, normalise, 0)

    pl.semaphore_wait(barrier, slabs + groups - 2)

    halos = []
    for side, step in ((0, slabs - 1), (1, 1)):
        copy = pltpu.make_async_remote_copy(
            src_ref=halo_out.at[side], dst_ref=halo_in.at[side],
            send_sem=halo_sem.at[0, side], recv_sem=halo_sem.at[1, side],
            device_id={"depth": lax.rem(depth + step, slabs)}, device_id_type=MESH)
        copy.start()
        halos.append(copy)
    for copy in halos:
        copy.wait()

    fold_mask = col < cols - width
    has_high = depth < slabs - 1
    has_low = depth > 0

    def filtered(p, energies):
        energies = list(energies)
        from_high = jnp.where(has_high, halo_in[0, p], 0.0)
        from_low = jnp.where(has_low, halo_in[1, p], 0.0)
        for i in range(rows_per_pack):
            r = p * rows_per_pack + i
            owner = p * (rows_per_pack // owned) + i // owned
            for s in range(shots):
                lows = []
                highs = []
                for c in range(tiles):
                    k = (i * shots + s) * tiles + c
                    lows.append(pltpu.roll(from_low, (LANES - k) % LANES, 1))
                    highs.append(pltpu.roll(from_high, LANES - 1 - k, 1))
                value = norm[s, r + 1, pl.ds(SUBLANES, cols)]
                beside = norm[s, r + 2, pl.ds(SUBLANES, cols)] + norm[s, r, pl.ds(SUBLANES, cols)]
                beside = beside + norm[s, r + 1, pl.ds(SUBLANES + 1, cols)]
                beside = beside + norm[s, r + 1, pl.ds(SUBLANES - 1, cols)]
                before = jnp.where(lane_row == 0, jnp.concatenate(lows, axis=0), pltpu.roll(value, 1, 1))
                after = jnp.where(lane_row == slab - 1, jnp.concatenate(highs, axis=0), pltpu.roll(value, slab - 1, 1))
                result = 6.0 * value - (beside + before + after)
                energies[s] = energies[s] + result * result
                other = pltpu.roll(result, cols - width, 0)
                folded = result + jnp.where(fold_mask, other, 0.0)
                send[owner, pl.ds((s * owned + i % owned) * width, width)] = folded[:width]
        return tuple(energies)

    energies = lax.fori_loop(0, packs, filtered, (plane,) * shots)

    order = sorted(range(1, groups), key=lambda j: abs(2 * j - groups))
    bulk = {}
    for j in order:
        target = lax.rem(group + j, groups)
        copy = pltpu.make_async_remote_copy(
            src_ref=send.at[target], dst_ref=recv.at[j - 1],
            send_sem=bulk_send.at[j - 1], recv_sem=bulk_recv.at[j - 1],
            device_id={"shot": target}, device_id_type=MESH)
        copy.start()
        bulk[j] = copy

    def total(value):
        return jnp.sum(jnp.sum(value, axis=0, keepdims=True), axis=1, keepdims=True)

    shot_row = lax.broadcasted_iota(jnp.int32, note_out.shape, 0)
    message = jnp.zeros(note_out.shape, jnp.float32)
    for s in range(shots):
        message = jnp.where(shot_row == s, total(energies[s]), message)
    energy_out[...] = message
    copies = []
    for j in range(1, slabs):
        copy = pltpu.make_async_remote_copy(
            src_ref=energy_out, dst_ref=energy_in.at[j - 1],
            send_sem=energy_send.at[j - 1], recv_sem=energy_recv.at[j - 1],
            device_id={"depth": lax.rem(depth + j, slabs)}, device_id_type=MESH)
        copy.start()
        copies.append(copy)
    for j, copy in enumerate(copies):
        copy.wait()
        message = message + energy_in[j]
    message = message / cells
    for s in range(shots):
        message = jnp.where(shot_row == shots + s, (box[s, 2] - 1).astype(jnp.float32), message)
    note_out[...] = message
    notes = {}
    for j in order:
        copy = pltpu.make_async_remote_copy(
            src_ref=note_out, dst_ref=note_in.at[j - 1],
            send_sem=note_send.at[j - 1], recv_sem=note_recv.at[j - 1],
            device_id={"shot": lax.rem(group + j, groups)}, device_id_type=MESH)
        copy.start()
        notes[j] = copy
    for j in order:
        notes[j].wait()
    peak = jnp.where(shot_row < shots, message, 0.0)
    for j in range(1, groups):
        peak = jnp.maximum(peak, jnp.where(shot_row < shots, note_in[j - 1], 0.0))
    peak = jnp.max(peak, axis=0, keepdims=True)

    scale = 1.0 / math.sqrt(total_shots)
    col_float = col.astype(jnp.float32)

    def unfold(block, note, sums):
        weight = scale / jnp.sqrt(note + 0.5 * peak + 1.0)
        for s in range(shots):
            first = note[shots + s:shots + s + 1]
            inside = (col_float >= first) & (col_float < first + width)
            factor = jnp.where(inside, weight[s:s + 1], 0.0)
            for i in range(owned):
                value = block[pl.ds((s * owned + i) * width, width)]
                sums[i] = sums[i] + factor * jnp.concatenate([value, value[:cols - width]], axis=0)
        return sums

    sums = unfold(send.at[group], message, [plane] * owned)
    for j in reversed(order):
        bulk[j].wait()
        sums = unfold(recv.at[j - 1], note_in[j - 1], sums)
    for i in range(owned):
        out_ref[i] = sums[i]


def on_device(correlation, illumination, aperture):
    shots, rows, cols, slab = correlation.shape
    groups = lax.axis_size("shot")
    slabs = lax.axis_size("depth")
    owned = rows // groups
    width = min(cols, cols // 2 + 2)
    dims = (shots, rows, cols, slab, groups, slabs, owned, width, shots * groups, rows * cols * slab * slabs)
    packs = rows * shots * (cols // SUBLANES) // LANES
    note_rows = -(-2 * shots // SUBLANES) * SUBLANES
    block = (shots * owned * width, slab)
    f32 = jnp.float32
    dma = pltpu.SemaphoreType.DMA
    return pl.pallas_call(
        functools.partial(kernel, dims),
        out_shape=jax.ShapeDtypeStruct((owned, cols, slab), f32),
        in_specs=[
            pl.BlockSpec(memory_space=pl.ANY),
            pl.BlockSpec(memory_space=pl.ANY),
            pl.BlockSpec(memory_space=pltpu.SMEM),
        ],
        out_specs=pl.BlockSpec(memory_space=pltpu.VMEM),
        scratch_shapes=[
            pltpu.VMEM((shots, rows, cols, slab), f32),
            pltpu.VMEM((shots, rows, cols, slab), f32),
            pltpu.VMEM((shots, rows + 2, cols + 2 * SUBLANES, slab), f32),
            pltpu.VMEM((2, packs, SUBLANES, LANES), f32),
            pltpu.VMEM((2, packs, SUBLANES, LANES), f32),
            pltpu.VMEM((groups,) + block, f32),
            pltpu.VMEM((groups - 1,) + block, f32),
            pltpu.VMEM((note_rows, LANES), f32),
            pltpu.VMEM((slabs - 1, note_rows, LANES), f32),
            pltpu.VMEM((note_rows, LANES), f32),
            pltpu.VMEM((groups - 1, note_rows, LANES), f32),
            dma((2, shots)),
            dma((2, 2)),
            dma((groups - 1,)),
            dma((groups - 1,)),
            dma((slabs - 1,)),
            dma((slabs - 1,)),
            dma((groups - 1,)),
            dma((groups - 1,)),
        ],
        compiler_params=pltpu.CompilerParams(collective_id=0, has_side_effects=True),
    )(correlation, illumination, aperture)


def solution(mesh):
    return jax.shard_map(
        on_device,
        mesh=mesh,
        in_specs=(P("shot", None, None, "depth"), P("shot", None, None, "depth"), P("shot", None)),
        out_specs=P("shot", None, "depth"),
        check_vma=False,
    )
```

```python
import functools
import math

import jax
import jax.numpy as jnp
from jax import lax
from jax.experimental import pallas as pl
from jax.experimental.pallas import tpu as pltpu
from jax.sharding import PartitionSpec as P

MESH = pl.DeviceIdType.MESH
LANES = 128
SUBLANES = 8
AHEAD = None


def kernel(dims, corr_hbm, ill_hbm, box, out_ref, corr, ill, norm, edge_out, edge_in, send, recv,
           note_out, note_in, load_sem, edge_send, edge_recv, bulk_send, bulk_recv, note_send, note_recv):
    shots, rows, cols, slab, groups, slabs, owned, width, total_shots, cells = dims
    tiles = cols // SUBLANES
    per_row = shots * tiles
    rows_per_pack = LANES // per_row
    packs = rows // rows_per_pack
    per_owner = owned * per_row
    owners_per_pack = LANES // per_owner
    group = lax.axis_index("shot")
    depth = lax.axis_index("depth")

    barrier = pltpu.get_barrier_semaphore()
    for j in range(1, groups):
        pl.semaphore_signal(barrier, inc=1, device_id={"shot": lax.rem(group + j, groups)}, device_id_type=MESH)
    for j in range(1, slabs):
        pl.semaphore_signal(barrier, inc=1, device_id={"depth": lax.rem(depth + j, slabs)}, device_id_type=MESH)

    loads = []
    for s in range(shots):
        pair = (
            pltpu.make_async_copy(corr_hbm.at[s], corr.at[s], load_sem.at[0, s]),
            pltpu.make_async_copy(ill_hbm.at[s], ill.at[s], load_sem.at[1, s]),
        )
        for copy in pair:
            copy.start()
        loads.append(pair)

    lane = lax.broadcasted_iota(jnp.int32, (SUBLANES, LANES), 1)
    lane_row = lax.broadcasted_iota(jnp.int32, (cols, slab), 1)
    col = lax.broadcasted_iota(jnp.int32, (cols, slab), 0)
    plane = jnp.zeros((cols, slab), jnp.float32)
    edge = jnp.zeros((SUBLANES, slab), jnp.float32)
    for s in range(shots):
        norm[s, 0, pl.ds(SUBLANES, cols)] = plane
        norm[s, rows + 1, pl.ds(SUBLANES, cols)] = plane

    col_mask = [(col >= box[s, 2]) & (col < box[s, 3]) for s in range(shots)]
    for pair in loads:
        for copy in pair:
            copy.wait()

    def pack(value, i, s, low, high):
        for c in range(tiles):
            k = (i * shots + s) * tiles + c
            piece = value[c * SUBLANES:(c + 1) * SUBLANES]
            low = jnp.where(lane == k, pltpu.roll(piece, k, 1), low)
            high = jnp.where(lane == k, pltpu.roll(piece, (k + 1) % LANES, 1), high)
        return low, high

    def normalise(p, carry):
        low = edge
        high = edge
        for i in range(rows_per_pack):
            r = p * rows_per_pack + i
            for s in range(shots):
                inside = col_mask[s] & (r >= box[s, 0]) & (r < box[s, 1])
                value = jnp.where(inside, corr[s, r], 0.0) / (ill[s, r] + 0.1)
                norm[s, r + 1, pl.ds(0, SUBLANES)] = edge
                norm[s, r + 1, pl.ds(SUBLANES, cols)] = value
                norm[s, r + 1, pl.ds(SUBLANES + cols, SUBLANES)] = edge
                low, high = pack(value, i, s, low, high)
        edge_out[p] = low
        edge_out[packs + p] = high
        return carry

    lax.fori_loop(0, packs, normalise, 0)

    fold_mask = col < cols - width
    not_first = lane_row > 0
    not_last = lane_row < slab - 1

    def filtered(p, energies):
        energies = list(energies)
        low = edge
        high = edge
        for i in range(rows_per_pack):
            r = p * rows_per_pack + i
            owner = p * (rows_per_pack // owned) + i // owned
            for s in range(shots):
                value = norm[s, r + 1, pl.ds(SUBLANES, cols)]
                beside = norm[s, r + 2, pl.ds(SUBLANES, cols)] + norm[s, r, pl.ds(SUBLANES, cols)]
                beside = beside + norm[s, r + 1, pl.ds(SUBLANES + 1, cols)]
                beside = beside + norm[s, r + 1, pl.ds(SUBLANES - 1, cols)]
                before = jnp.where(not_first, pltpu.roll(value, 1, 1), 0.0)
                after = jnp.where(not_last, pltpu.roll(value, slab - 1, 1), 0.0)
                result = 6.0 * value - (beside + before + after)
                energies[s] = energies[s] + result * result
                low, high = pack(result, i, s, low, high)
                other = pltpu.roll(result, cols - width, 0)
                folded = result + jnp.where(fold_mask, other, 0.0)
                send[owner, pl.ds((s * owned + i % owned) * width, width)] = folded[:width]
        edge_out[2 * packs + p] = low
        edge_out[3 * packs + p] = high
        return tuple(energies)

    energies = lax.fori_loop(0, packs, filtered, (plane,) * shots)

    def total(value):
        return jnp.sum(jnp.sum(value, axis=0, keepdims=True), axis=1, keepdims=True)

    shot_row = lax.broadcasted_iota(jnp.int32, (SUBLANES, LANES), 0)
    message = edge
    for s in range(shots):
        message = jnp.where(shot_row == s, total(energies[s]), message)
    edge_out[4 * packs] = message

    pl.semaphore_wait(barrier, slabs + groups - 2)

    edges = []
    for j in range(1, slabs):
        copy = pltpu.make_async_remote_copy(
            src_ref=edge_out, dst_ref=edge_in.at[j - 1],
            send_sem=edge_send.at[j - 1], recv_sem=edge_recv.at[j - 1],
            device_id={"depth": lax.rem(depth + j, slabs)}, device_id_type=MESH)
        copy.start()
        edges.append(copy)

    order = sorted(range(1, groups), key=lambda j: abs(2 * j - groups))
    ahead = len(order) if AHEAD is None else min(AHEAD, len(order))
    bulk = {}
    for j in order:
        target = lax.rem(group + j, groups)
        bulk[j] = pltpu.make_async_remote_copy(
            src_ref=send.at[target], dst_ref=recv.at[j - 1],
            send_sem=bulk_send.at[j - 1], recv_sem=bulk_recv.at[j - 1],
            device_id={"shot": target}, device_id_type=MESH)
    for j in order[:ahead]:
        bulk[j].start()

    for copy in edges:
        copy.wait()
    places = [edge_out] + [edge_in.at[slabs - i - 1] for i in range(1, slabs)]
    for i in range(1, slabs):
        message = message + places[i][4 * packs]
    cross = edge
    for i in range(slabs):
        here, there = places[i], places[(i + 1) % slabs]
        part = edge
        for p in range(packs):
            above = there[p]
            below = here[packs + p]
            part = part + above * (above - 2.0 * here[3 * packs + p])
            part = part + below * (below - 2.0 * there[2 * packs + p])
        cross = cross + jnp.where(lax.rem(depth + i, slabs) < slabs - 1, part, 0.0)
    lane_shot = lax.rem(lane // tiles, shots)
    for s in range(shots):
        message = message + jnp.where(shot_row == s, total(jnp.where(lane_shot == s, cross, 0.0)), 0.0)
    message = message / cells
    for s in range(shots):
        message = jnp.where(shot_row == shots + s, (box[s, 2] - 1).astype(jnp.float32), message)
    for p in range(packs):
        low = jnp.where(depth > 0, places[slabs - 1][packs + p], 0.0)
        high = jnp.where(depth < slabs - 1, places[1][p], 0.0)
        for q in range(owners_per_pack):
            offset = q * per_owner
            halo = jnp.where(lane < per_owner, pltpu.roll(low, (LANES - offset) % LANES, 1),
                             pltpu.roll(high, (LANES + per_owner - offset) % LANES, 1))
            owner = p * owners_per_pack + q
            note_out[owner, 0] = jnp.where(lane < 2 * per_owner, halo, 0.0)
            note_out[owner, 1] = message
    notes = {}
    for j in order:
        target = lax.rem(group + j, groups)
        notes[j] = pltpu.make_async_remote_copy(
            src_ref=note_out.at[target], dst_ref=note_in.at[j - 1],
            send_sem=note_send.at[j - 1], recv_sem=note_recv.at[j - 1],
            device_id={"shot": target}, device_id_type=MESH)
        notes[j].start()
    for j in order[ahead:]:
        bulk[j].start()
    for j in order:
        notes[j].wait()
    peak = jnp.where(shot_row < shots, message, 0.0)
    for j in range(1, groups):
        peak = jnp.maximum(peak, jnp.where(shot_row < shots, note_in[j - 1, 1], 0.0))
    peak = jnp.max(peak, axis=0, keepdims=True)

    scale = 1.0 / math.sqrt(total_shots)
    col_float = col.astype(jnp.float32)

    def unfold(block, note, sums):
        row = note[1]
        weight = scale / jnp.sqrt(jnp.where(shot_row < shots, row, 0.0) + 0.5 * peak + 1.0)
        by_lane = edge
        for s in range(shots):
            first = row[shots + s:shots + s + 1]
            inside = (col_float >= first) & (col_float < first + width)
            factor = jnp.where(inside, weight[s:s + 1], 0.0)
            by_lane = jnp.where(lane_shot == s, weight[s:s + 1], by_lane)
            for i in range(owned):
                value = block[pl.ds((s * owned + i) * width, width)]
                sums[i] = sums[i] + factor * jnp.concatenate([value, value[:cols - width]], axis=0)
        sums[owned] = sums[owned] + by_lane * note[0]
        return sums

    sums = unfold(send.at[group], note_out.at[group], [plane] * owned + [edge])
    for j in order[:ahead][::-1] + order[ahead:]:
        bulk[j].wait()
        sums = unfold(recv.at[j - 1], note_in.at[j - 1], sums)
    halo = sums[owned]
    for s in range(1, shots):
        halo = halo + pltpu.roll(sums[owned], LANES - s * tiles, 1)
    for i in range(owned):
        lows = []
        highs = []
        for c in range(tiles):
            k = i * per_row + c
            lows.append(pltpu.roll(halo, (LANES - k) % LANES, 1))
            highs.append(pltpu.roll(halo, LANES - 1 - per_owner - k, 1))
        value = sums[i] - jnp.where(not_first, 0.0, jnp.concatenate(lows, axis=0))
        out_ref[i] = value - jnp.where(not_last, 0.0, jnp.concatenate(highs, axis=0))


def on_device(correlation, illumination, aperture):
    shots, rows, cols, slab = correlation.shape
    groups = lax.axis_size("shot")
    slabs = lax.axis_size("depth")
    owned = rows // groups
    width = min(cols, cols // 2 + 2)
    dims = (shots, rows, cols, slab, groups, slabs, owned, width, shots * groups, rows * cols * slab * slabs)
    packs = rows * shots * (cols // SUBLANES) // LANES
    edges = (4 * packs + 1, SUBLANES, LANES)
    block = (shots * owned * width, slab)
    f32 = jnp.float32
    dma = pltpu.SemaphoreType.DMA
    return pl.pallas_call(
        functools.partial(kernel, dims),
        out_shape=jax.ShapeDtypeStruct((owned, cols, slab), f32),
        in_specs=[
            pl.BlockSpec(memory_space=pl.ANY),
            pl.BlockSpec(memory_space=pl.ANY),
            pl.BlockSpec(memory_space=pltpu.SMEM),
        ],
        out_specs=pl.BlockSpec(memory_space=pltpu.VMEM),
        scratch_shapes=[
            pltpu.VMEM((shots, rows, cols, slab), f32),
            pltpu.VMEM((shots, rows, cols, slab), f32),
            pltpu.VMEM((shots, rows + 2, cols + 2 * SUBLANES, slab), f32),
            pltpu.VMEM(edges, f32),
            pltpu.VMEM((slabs - 1,) + edges, f32),
            pltpu.VMEM((groups,) + block, f32),
            pltpu.VMEM((groups - 1,) + block, f32),
            pltpu.VMEM((groups, 2, SUBLANES, LANES), f32),
            pltpu.VMEM((groups - 1, 2, SUBLANES, LANES), f32),
            dma((2, shots)),
            dma((slabs - 1,)),
            dma((slabs - 1,)),
            dma((groups - 1,)),
            dma((groups - 1,)),
            dma((groups - 1,)),
            dma((groups - 1,)),
        ],
        compiler_params=pltpu.CompilerParams(collective_id=0, has_side_effects=True),
    )(correlation, illumination, aperture)


def solution(mesh):
    return jax.shard_map(
        on_device,
        mesh=mesh,
        in_specs=(P("shot", None, None, "depth"), P("shot", None, None, "depth"), P("shot", None)),
        out_specs=P("shot", None, "depth"),
        check_vma=False,
    )
```

```python
import functools
import math

import jax
import jax.numpy as jnp
from jax import lax
from jax.experimental import pallas as pl
from jax.experimental.pallas import tpu as pltpu
from jax.sharding import PartitionSpec as P

MESH = pl.DeviceIdType.MESH
LANES = 128
SUBLANES = 8
NEAR = 2


def kernel(dims, corr_hbm, ill_hbm, box, out_ref, corr, ill, norm, edge_out, edge_in, send, recv,
           note_out, note_in, load_sem, edge_send, edge_recv, bulk_send, bulk_recv, note_send, note_recv):
    shots, rows, cols, slab, groups, slabs, owned, width, total_shots, cells = dims
    tiles = cols // SUBLANES
    per_row = shots * tiles
    rows_per_pack = LANES // per_row
    packs = rows // rows_per_pack
    per_owner = owned * per_row
    owners_per_pack = LANES // per_owner
    group = lax.axis_index("shot")
    depth = lax.axis_index("depth")

    barrier = pltpu.get_barrier_semaphore()
    for j in range(1, groups):
        pl.semaphore_signal(barrier, inc=1, device_id={"shot": lax.rem(group + j, groups)}, device_id_type=MESH)
    for j in range(1, slabs):
        pl.semaphore_signal(barrier, inc=1, device_id={"depth": lax.rem(depth + j, slabs)}, device_id_type=MESH)

    loads = []
    for s in range(shots):
        pair = (
            pltpu.make_async_copy(corr_hbm.at[s], corr.at[s], load_sem.at[0, s]),
            pltpu.make_async_copy(ill_hbm.at[s], ill.at[s], load_sem.at[1, s]),
        )
        for copy in pair:
            copy.start()
        loads.append(pair)

    lane = lax.broadcasted_iota(jnp.int32, (SUBLANES, LANES), 1)
    lane_row = lax.broadcasted_iota(jnp.int32, (cols, slab), 1)
    col = lax.broadcasted_iota(jnp.int32, (cols, slab), 0)
    plane = jnp.zeros((cols, slab), jnp.float32)
    edge = jnp.zeros((SUBLANES, slab), jnp.float32)
    for s in range(shots):
        norm[s, 0, pl.ds(SUBLANES, cols)] = plane
        norm[s, rows + 1, pl.ds(SUBLANES, cols)] = plane

    col_mask = [(col >= box[s, 2]) & (col < box[s, 3]) for s in range(shots)]
    for pair in loads:
        for copy in pair:
            copy.wait()

    def pack(value, i, s, low, high):
        for c in range(tiles):
            k = (i * shots + s) * tiles + c
            piece = value[c * SUBLANES:(c + 1) * SUBLANES]
            low = jnp.where(lane == k, pltpu.roll(piece, k, 1), low)
            high = jnp.where(lane == k, pltpu.roll(piece, (k + 1) % LANES, 1), high)
        return low, high

    def normalise(p, carry):
        low = edge
        high = edge
        for i in range(rows_per_pack):
            r = p * rows_per_pack + i
            for s in range(shots):
                inside = col_mask[s] & (r >= box[s, 0]) & (r < box[s, 1])
                value = jnp.where(inside, corr[s, r], 0.0) / (ill[s, r] + 0.1)
                norm[s, r + 1, pl.ds(0, SUBLANES)] = edge
                norm[s, r + 1, pl.ds(SUBLANES, cols)] = value
                norm[s, r + 1, pl.ds(SUBLANES + cols, SUBLANES)] = edge
                low, high = pack(value, i, s, low, high)
        edge_out[p] = low
        edge_out[packs + p] = high
        return carry

    lax.fori_loop(0, packs, normalise, 0)

    fold_mask = col < cols - width
    not_first = lane_row > 0
    not_last = lane_row < slab - 1

    def filtered(p, energies):
        energies = list(energies)
        low = edge
        high = edge
        for i in range(rows_per_pack):
            r = p * rows_per_pack + i
            owner = p * (rows_per_pack // owned) + i // owned
            for s in range(shots):
                value = norm[s, r + 1, pl.ds(SUBLANES, cols)]
                beside = norm[s, r + 2, pl.ds(SUBLANES, cols)] + norm[s, r, pl.ds(SUBLANES, cols)]
                beside = beside + norm[s, r + 1, pl.ds(SUBLANES + 1, cols)]
                beside = beside + norm[s, r + 1, pl.ds(SUBLANES - 1, cols)]
                before = jnp.where(not_first, pltpu.roll(value, 1, 1), 0.0)
                after = jnp.where(not_last, pltpu.roll(value, slab - 1, 1), 0.0)
                result = 6.0 * value - (beside + before + after)
                energies[s] = energies[s] + result * result
                low, high = pack(result, i, s, low, high)
                other = pltpu.roll(result, cols - width, 0)
                folded = result + jnp.where(fold_mask, other, 0.0)
                send[owner, pl.ds((s * owned + i % owned) * width, width)] = folded[:width]
        edge_out[2 * packs + p] = low
        edge_out[3 * packs + p] = high
        return tuple(energies)

    energies = lax.fori_loop(0, packs, filtered, (plane,) * shots)

    def total(value):
        return jnp.sum(jnp.sum(value, axis=0, keepdims=True), axis=1, keepdims=True)

    shot_row = lax.broadcasted_iota(jnp.int32, (SUBLANES, LANES), 0)
    message = edge
    for s in range(shots):
        message = jnp.where(shot_row == s, total(energies[s]), message)
    edge_out[4 * packs] = message

    pl.semaphore_wait(barrier, slabs + groups - 2)

    edges = []
    for j in range(1, slabs):
        copy = pltpu.make_async_remote_copy(
            src_ref=edge_out, dst_ref=edge_in.at[j - 1],
            send_sem=edge_send.at[j - 1], recv_sem=edge_recv.at[j - 1],
            device_id={"depth": lax.rem(depth + j, slabs)}, device_id_type=MESH)
        copy.start()
        edges.append(copy)

    order = sorted(range(1, groups), key=lambda j: abs(2 * j - groups))
    pair = 2 if groups % 2 == 0 else 1

    def distance(j):
        target = lax.rem(group + j, groups)
        return jnp.abs(target // pair - group // pair) + jnp.abs(lax.rem(target, pair) - lax.rem(group, pair))

    def start_bulk(far):
        for level in range(3, -1, -1):
            if (level >= NEAR) == far:
                for j in order:
                    near = distance(j)
                    pl.when((near > level) & ((near <= level + 1) | (level == 3)))(bulk[j].start)

    bulk = {}
    for j in order:
        target = lax.rem(group + j, groups)
        bulk[j] = pltpu.make_async_remote_copy(
            src_ref=send.at[target], dst_ref=recv.at[j - 1],
            send_sem=bulk_send.at[j - 1], recv_sem=bulk_recv.at[j - 1],
            device_id={"shot": target}, device_id_type=MESH)
    start_bulk(True)

    for copy in edges:
        copy.wait()
    places = [edge_out] + [edge_in.at[slabs - i - 1] for i in range(1, slabs)]
    for i in range(1, slabs):
        message = message + places[i][4 * packs]
    cross = edge
    for i in range(slabs):
        here, there = places[i], places[(i + 1) % slabs]
        part = edge
        for p in range(packs):
            above = there[p]
            below = here[packs + p]
            part = part + above * (above - 2.0 * here[3 * packs + p])
            part = part + below * (below - 2.0 * there[2 * packs + p])
        cross = cross + jnp.where(lax.rem(depth + i, slabs) < slabs - 1, part, 0.0)
    lane_shot = lax.rem(lane // tiles, shots)
    for s in range(shots):
        message = message + jnp.where(shot_row == s, total(jnp.where(lane_shot == s, cross, 0.0)), 0.0)
    message = message / cells
    for s in range(shots):
        message = jnp.where(shot_row == shots + s, (box[s, 2] - 1).astype(jnp.float32), message)
    for p in range(packs):
        low = jnp.where(depth > 0, places[slabs - 1][packs + p], 0.0)
        high = jnp.where(depth < slabs - 1, places[1][p], 0.0)
        for q in range(owners_per_pack):
            offset = q * per_owner
            halo = jnp.where(lane < per_owner, pltpu.roll(low, (LANES - offset) % LANES, 1),
                             pltpu.roll(high, (LANES + per_owner - offset) % LANES, 1))
            owner = p * owners_per_pack + q
            note_out[owner, 0] = jnp.where(lane < 2 * per_owner, halo, 0.0)
            note_out[owner, 1] = message
    notes = {}
    for j in order:
        target = lax.rem(group + j, groups)
        notes[j] = pltpu.make_async_remote_copy(
            src_ref=note_out.at[target], dst_ref=note_in.at[j - 1],
            send_sem=note_send.at[j - 1], recv_sem=note_recv.at[j - 1],
            device_id={"shot": target}, device_id_type=MESH)
        notes[j].start()
    start_bulk(False)
    for j in order:
        notes[j].wait()
    peak = jnp.where(shot_row < shots, message, 0.0)
    for j in range(1, groups):
        peak = jnp.maximum(peak, jnp.where(shot_row < shots, note_in[j - 1, 1], 0.0))
    peak = jnp.max(peak, axis=0, keepdims=True)

    scale = 1.0 / math.sqrt(total_shots)
    col_float = col.astype(jnp.float32)

    def unfold(block, note, sums):
        row = note[1]
        weight = scale / jnp.sqrt(jnp.where(shot_row < shots, row, 0.0) + 0.5 * peak + 1.0)
        by_lane = edge
        for s in range(shots):
            first = row[shots + s:shots + s + 1]
            inside = (col_float >= first) & (col_float < first + width)
            factor = jnp.where(inside, weight[s:s + 1], 0.0)
            by_lane = jnp.where(lane_shot == s, weight[s:s + 1], by_lane)
            for i in range(owned):
                value = block[pl.ds((s * owned + i) * width, width)]
                sums[i] = sums[i] + factor * jnp.concatenate([value, value[:cols - width]], axis=0)
        sums[owned] = sums[owned] + by_lane * note[0]
        return sums

    sums = unfold(send.at[group], note_out.at[group], [plane] * owned + [edge])
    for j in order:
        bulk[j].wait()
        sums = unfold(recv.at[j - 1], note_in.at[j - 1], sums)
    halo = sums[owned]
    for s in range(1, shots):
        halo = halo + pltpu.roll(sums[owned], LANES - s * tiles, 1)
    for i in range(owned):
        lows = []
        highs = []
        for c in range(tiles):
            k = i * per_row + c
            lows.append(pltpu.roll(halo, (LANES - k) % LANES, 1))
            highs.append(pltpu.roll(halo, LANES - 1 - per_owner - k, 1))
        value = sums[i] - jnp.where(not_first, 0.0, jnp.concatenate(lows, axis=0))
        out_ref[i] = value - jnp.where(not_last, 0.0, jnp.concatenate(highs, axis=0))


def on_device(correlation, illumination, aperture):
    shots, rows, cols, slab = correlation.shape
    groups = lax.axis_size("shot")
    slabs = lax.axis_size("depth")
    owned = rows // groups
    width = min(cols, cols // 2 + 2)
    dims = (shots, rows, cols, slab, groups, slabs, owned, width, shots * groups, rows * cols * slab * slabs)
    packs = rows * shots * (cols // SUBLANES) // LANES
    edges = (4 * packs + 1, SUBLANES, LANES)
    block = (shots * owned * width, slab)
    f32 = jnp.float32
    dma = pltpu.SemaphoreType.DMA
    return pl.pallas_call(
        functools.partial(kernel, dims),
        out_shape=pltpu.VMEM((owned, cols, slab), f32),
        in_specs=[
            pl.BlockSpec(memory_space=pl.ANY),
            pl.BlockSpec(memory_space=pl.ANY),
            pl.BlockSpec(memory_space=pltpu.SMEM),
        ],
        out_specs=pl.BlockSpec(memory_space=pltpu.VMEM),
        scratch_shapes=[
            pltpu.VMEM((shots, rows, cols, slab), f32),
            pltpu.VMEM((shots, rows, cols, slab), f32),
            pltpu.VMEM((shots, rows + 2, cols + 2 * SUBLANES, slab), f32),
            pltpu.VMEM(edges, f32),
            pltpu.VMEM((slabs - 1,) + edges, f32),
            pltpu.VMEM((groups,) + block, f32),
            pltpu.VMEM((groups - 1,) + block, f32),
            pltpu.VMEM((groups, 2, SUBLANES, LANES), f32),
            pltpu.VMEM((groups - 1, 2, SUBLANES, LANES), f32),
            dma((2, shots)),
            dma((slabs - 1,)),
            dma((slabs - 1,)),
            dma((groups - 1,)),
            dma((groups - 1,)),
            dma((groups - 1,)),
            dma((groups - 1,)),
        ],
        compiler_params=pltpu.CompilerParams(collective_id=0, has_side_effects=True),
    )(correlation, illumination, aperture)


def solution(mesh):
    return jax.shard_map(
        on_device,
        mesh=mesh,
        in_specs=(P("shot", None, None, "depth"), P("shot", None, None, "depth"), P("shot", None)),
        out_specs=P("shot", None, "depth"),
        check_vma=False,
    )
```

```python
import functools
import math

import jax
import jax.numpy as jnp
from jax import lax
from jax.experimental import pallas as pl
from jax.experimental.pallas import tpu as pltpu
from jax.sharding import PartitionSpec as P

MESH = pl.DeviceIdType.MESH
LANES = 128
SUBLANES = 8
NEAR = 2


def kernel(dims, corr_hbm, ill_hbm, box, out_ref, corr, ill, norm, edge_out, edge_in, send, recv,
           note_out, note_in, load_sem, edge_send, edge_recv, bulk_send, bulk_recv, note_send, note_recv):
    shots, rows, cols, slab, groups, slabs, owned, width, total_shots, cells = dims
    tiles = cols // SUBLANES
    per_row = shots * tiles
    rows_per_pack = LANES // per_row
    packs = rows // rows_per_pack
    per_owner = owned * per_row
    owners_per_pack = LANES // per_owner
    group = lax.axis_index("shot")
    depth = lax.axis_index("depth")

    barrier = pltpu.get_barrier_semaphore()
    for j in range(1, groups):
        pl.semaphore_signal(barrier, inc=1, device_id={"shot": lax.rem(group + j, groups)}, device_id_type=MESH)
    for j in range(1, slabs):
        pl.semaphore_signal(barrier, inc=1, device_id={"depth": lax.rem(depth + j, slabs)}, device_id_type=MESH)

    loads = []
    for s in range(shots):
        pair = (
            pltpu.make_async_copy(corr_hbm.at[s], corr.at[s], load_sem.at[0, s]),
            pltpu.make_async_copy(ill_hbm.at[s], ill.at[s], load_sem.at[1, s]),
        )
        for copy in pair:
            copy.start()
        loads.append(pair)

    lane = lax.broadcasted_iota(jnp.int32, (SUBLANES, LANES), 1)
    lane_row = lax.broadcasted_iota(jnp.int32, (cols, slab), 1)
    col = lax.broadcasted_iota(jnp.int32, (cols, slab), 0)
    plane = jnp.zeros((cols, slab), jnp.float32)
    edge = jnp.zeros((SUBLANES, slab), jnp.float32)
    for s in range(shots):
        norm[s, 0, pl.ds(SUBLANES, cols)] = plane
        norm[s, rows + 1, pl.ds(SUBLANES, cols)] = plane

    col_mask = [(col >= box[s, 2]) & (col < box[s, 3]) for s in range(shots)]
    for pair in loads:
        for copy in pair:
            copy.wait()

    def pack(value, i, s, low, high):
        for c in range(tiles):
            k = (i * shots + s) * tiles + c
            piece = value[c * SUBLANES:(c + 1) * SUBLANES]
            low = jnp.where(lane == k, pltpu.roll(piece, k, 1), low)
            high = jnp.where(lane == k, pltpu.roll(piece, (k + 1) % LANES, 1), high)
        return low, high

    def normalise(p, carry):
        low = edge
        high = edge
        for i in range(rows_per_pack):
            r = p * rows_per_pack + i
            for s in range(shots):
                inside = col_mask[s] & (r >= box[s, 0]) & (r < box[s, 1])
                value = jnp.where(inside, corr[s, r], 0.0) / (ill[s, r] + 0.1)
                norm[s, r + 1, pl.ds(0, SUBLANES)] = edge
                norm[s, r + 1, pl.ds(SUBLANES, cols)] = value
                norm[s, r + 1, pl.ds(SUBLANES + cols, SUBLANES)] = edge
                low, high = pack(value, i, s, low, high)
        edge_out[p] = low
        edge_out[packs + p] = high
        return carry

    lax.fori_loop(0, packs, normalise, 0)

    fold_mask = col < cols - width
    not_first = lane_row > 0
    not_last = lane_row < slab - 1

    def filtered(p, energies):
        energies = list(energies)
        low = edge
        high = edge
        for i in range(rows_per_pack):
            r = p * rows_per_pack + i
            owner = p * (rows_per_pack // owned) + i // owned
            for s in range(shots):
                value = norm[s, r + 1, pl.ds(SUBLANES, cols)]
                beside = norm[s, r + 2, pl.ds(SUBLANES, cols)] + norm[s, r, pl.ds(SUBLANES, cols)]
                beside = beside + norm[s, r + 1, pl.ds(SUBLANES + 1, cols)]
                beside = beside + norm[s, r + 1, pl.ds(SUBLANES - 1, cols)]
                before = jnp.where(not_first, pltpu.roll(value, 1, 1), 0.0)
                after = jnp.where(not_last, pltpu.roll(value, slab - 1, 1), 0.0)
                result = 6.0 * value - (beside + before + after)
                energies[s] = energies[s] + result * result
                low, high = pack(result, i, s, low, high)
                other = pltpu.roll(result, cols - width, 0)
                folded = result + jnp.where(fold_mask, other, 0.0)
                send[owner, pl.ds((s * owned + i % owned) * width, width)] = folded[:width]
        edge_out[2 * packs + p] = low
        edge_out[3 * packs + p] = high
        return tuple(energies)

    energies = lax.fori_loop(0, packs, filtered, (plane,) * shots)

    def total(value):
        return jnp.sum(jnp.sum(value, axis=0, keepdims=True), axis=1, keepdims=True)

    shot_row = lax.broadcasted_iota(jnp.int32, (SUBLANES, LANES), 0)
    message = edge
    for s in range(shots):
        message = jnp.where(shot_row == s, total(energies[s]), message)
    edge_out[4 * packs] = message

    pl.semaphore_wait(barrier, slabs + groups - 2)

    edges = []
    for j in range(1, slabs):
        copy = pltpu.make_async_remote_copy(
            src_ref=edge_out, dst_ref=edge_in.at[j - 1],
            send_sem=edge_send.at[j - 1], recv_sem=edge_recv.at[j - 1],
            device_id={"depth": lax.rem(depth + j, slabs)}, device_id_type=MESH)
        copy.start()
        edges.append(copy)

    order = sorted(range(1, groups), key=lambda j: abs(2 * j - groups))
    pair = 2 if groups % 2 == 0 else 1

    def distance(j):
        target = lax.rem(group + j, groups)
        return jnp.abs(target // pair - group // pair) + jnp.abs(lax.rem(target, pair) - lax.rem(group, pair))

    def start_bulk(far):
        for level in range(3, -1, -1):
            if (level >= NEAR) == far:
                for j in order:
                    near = distance(j)
                    pl.when((near > level) & ((near <= level + 1) | (level == 3)))(bulk[j].start)

    bulk = {}
    for j in order:
        target = lax.rem(group + j, groups)
        bulk[j] = pltpu.make_async_remote_copy(
            src_ref=send.at[target], dst_ref=recv.at[j - 1],
            send_sem=bulk_send.at[j - 1], recv_sem=bulk_recv.at[j - 1],
            device_id={"shot": target}, device_id_type=MESH)
    start_bulk(True)

    for copy in edges:
        copy.wait()
    places = [edge_out] + [edge_in.at[slabs - i - 1] for i in range(1, slabs)]
    for i in range(1, slabs):
        message = message + places[i][4 * packs]
    cross = edge
    for i in range(slabs):
        here, there = places[i], places[(i + 1) % slabs]
        part = edge
        for p in range(packs):
            above = there[p]
            below = here[packs + p]
            part = part + above * (above - 2.0 * here[3 * packs + p])
            part = part + below * (below - 2.0 * there[2 * packs + p])
        cross = cross + jnp.where(lax.rem(depth + i, slabs) < slabs - 1, part, 0.0)
    lane_shot = lax.rem(lane // tiles, shots)
    for s in range(shots):
        message = message + jnp.where(shot_row == s, total(jnp.where(lane_shot == s, cross, 0.0)), 0.0)
    message = message / cells
    for s in range(shots):
        message = jnp.where(shot_row == shots + s, (box[s, 2] - 1).astype(jnp.float32), message)
    for p in range(packs):
        low = jnp.where(depth > 0, places[slabs - 1][packs + p], 0.0)
        high = jnp.where(depth < slabs - 1, places[1][p], 0.0)
        for q in range(owners_per_pack):
            offset = q * per_owner
            halo = jnp.where(lane < per_owner, pltpu.roll(low, (LANES - offset) % LANES, 1),
                             pltpu.roll(high, (LANES + per_owner - offset) % LANES, 1))
            owner = p * owners_per_pack + q
            note_out[owner, 0] = jnp.where(lane < 2 * per_owner, halo, 0.0)
            note_out[owner, 1] = message
    notes = {}
    for j in order:
        target = lax.rem(group + j, groups)
        notes[j] = pltpu.make_async_remote_copy(
            src_ref=note_out.at[target], dst_ref=note_in.at[j - 1],
            send_sem=note_send.at[j - 1], recv_sem=note_recv.at[j - 1],
            device_id={"shot": target}, device_id_type=MESH)
    for level in range(3, -1, -1):
        for j in order:
            near = distance(j)
            pl.when((near > level) & ((near <= level + 1) | (level == 3)))(notes[j].start)
    start_bulk(False)
    for j in order:
        notes[j].wait()
    peak = jnp.where(shot_row < shots, message, 0.0)
    for j in range(1, groups):
        peak = jnp.maximum(peak, jnp.where(shot_row < shots, note_in[j - 1, 1], 0.0))
    peak = jnp.max(peak, axis=0, keepdims=True)

    scale = 1.0 / math.sqrt(total_shots)
    col_float = col.astype(jnp.float32)

    def unfold(block, note, sums):
        row = note[1]
        weight = scale / jnp.sqrt(jnp.where(shot_row < shots, row, 0.0) + 0.5 * peak + 1.0)
        by_lane = edge
        for s in range(shots):
            first = row[shots + s:shots + s + 1]
            inside = (col_float >= first) & (col_float < first + width)
            factor = jnp.where(inside, weight[s:s + 1], 0.0)
            by_lane = jnp.where(lane_shot == s, weight[s:s + 1], by_lane)
            for i in range(owned):
                value = block[pl.ds((s * owned + i) * width, width)]
                sums[i] = sums[i] + factor * jnp.concatenate([value, value[:cols - width]], axis=0)
        sums[owned] = sums[owned] + by_lane * note[0]
        return sums

    sums = unfold(send.at[group], note_out.at[group], [plane] * owned + [edge])
    for j in order:
        bulk[j].wait()
        sums = unfold(recv.at[j - 1], note_in.at[j - 1], sums)
    halo = sums[owned]
    for s in range(1, shots):
        halo = halo + pltpu.roll(sums[owned], LANES - s * tiles, 1)
    for i in range(owned):
        lows = []
        highs = []
        for c in range(tiles):
            k = i * per_row + c
            lows.append(pltpu.roll(halo, (LANES - k) % LANES, 1))
            highs.append(pltpu.roll(halo, LANES - 1 - per_owner - k, 1))
        value = sums[i] - jnp.where(not_first, 0.0, jnp.concatenate(lows, axis=0))
        out_ref[i] = value - jnp.where(not_last, 0.0, jnp.concatenate(highs, axis=0))


def on_device(correlation, illumination, aperture):
    shots, rows, cols, slab = correlation.shape
    groups = lax.axis_size("shot")
    slabs = lax.axis_size("depth")
    owned = rows // groups
    width = min(cols, cols // 2 + 2)
    dims = (shots, rows, cols, slab, groups, slabs, owned, width, shots * groups, rows * cols * slab * slabs)
    packs = rows * shots * (cols // SUBLANES) // LANES
    edges = (4 * packs + 1, SUBLANES, LANES)
    block = (shots * owned * width, slab)
    f32 = jnp.float32
    dma = pltpu.SemaphoreType.DMA
    return pl.pallas_call(
        functools.partial(kernel, dims),
        out_shape=pltpu.VMEM((owned, cols, slab), f32),
        in_specs=[
            pl.BlockSpec(memory_space=pl.ANY),
            pl.BlockSpec(memory_space=pl.ANY),
            pl.BlockSpec(memory_space=pltpu.SMEM),
        ],
        out_specs=pl.BlockSpec(memory_space=pltpu.VMEM),
        scratch_shapes=[
            pltpu.VMEM((shots, rows, cols, slab), f32),
            pltpu.VMEM((shots, rows, cols, slab), f32),
            pltpu.VMEM((shots, rows + 2, cols + 2 * SUBLANES, slab), f32),
            pltpu.VMEM(edges, f32),
            pltpu.VMEM((slabs - 1,) + edges, f32),
            pltpu.VMEM((groups,) + block, f32),
            pltpu.VMEM((groups - 1,) + block, f32),
            pltpu.VMEM((groups, 2, SUBLANES, LANES), f32),
            pltpu.VMEM((groups - 1, 2, SUBLANES, LANES), f32),
            dma((2, shots)),
            dma((slabs - 1,)),
            dma((slabs - 1,)),
            dma((groups - 1,)),
            dma((groups - 1,)),
            dma((groups - 1,)),
            dma((groups - 1,)),
        ],
        compiler_params=pltpu.CompilerParams(collective_id=0, has_side_effects=True),
    )(correlation, illumination, aperture)


def solution(mesh):
    return jax.shard_map(
        on_device,
        mesh=mesh,
        in_specs=(P("shot", None, None, "depth"), P("shot", None, None, "depth"), P("shot", None)),
        out_specs=P("shot", None, "depth"),
        check_vma=False,
    )
```
